32 devices in a mesh: gx: 2 (over core), gy: 4 (over y, x), gz: 4 (over z).
Axes of the slice: x: 2, y: 2, z: 4, core: 2. Of those that a mesh axis runs over, the one named last changes fastest.
Arguments:
- block_values: bfloat16 [4, 64, 4, 6, 128, 128], P('gy', 'gx', 'gz'), as said below
- block_cols: int32 [4, 64, 4, 6], P('gy', 'gx', 'gz'), may hold values from 0 to 63, as said below
Outputs:
- purified: float32 [256, 32768], P(('gx', 'gy'), 'gz')
The draws below stay inside these ranges and needn't reach their ends.
Inputs may be any that keep to these rules, and one draw needn't show every extreme that they name: block_cols[a, s, b, :] holds 6 distinct tile columns of panel b at which tile row a * 64 + s of P is nonzero; every tile column of a panel is listed by exactly 6 tile rows of each slab; the pattern is symmetric: tile (i, j) is listed exactly when tile (j, i) is. `block_values`: P is symmetric: the tile listed at (i, j) is the transpose of the tile listed at (j, i), and diagonal tiles are symmetric.
All inputs are finite; a program needn't handle non-finite values.
Results may differ from the reference program's by a relative error of at most 0.0033.
Values may be sent and summed in bfloat16 or wider, within the bound.
A program may use at most 128 MiB of HBM per device.

```python
import jax
import jax.numpy as jnp
from jax import lax

TILE = 128
NT = 256
KP = 6
WIN = 1
NPAN = 4
ST = 64
RB = 32
ORDER = 32768
N_GX = 2


def tile_pattern(key):
    pattern_key = jax.random.fold_in(key, 11)
    split_keys = jax.random.split(pattern_key, 2)
    order_keys = jax.random.split(split_keys[0], NPAN * NPAN * 2)
    orders = jax.vmap(lambda subkey: jax.random.permutation(subkey, ST))(order_keys).reshape(NPAN, NPAN, 2, ST)
    first = orders[:, :, 0].astype(jnp.int32)
    second = orders[:, :, 1].astype(jnp.int32)
    slab_index = jnp.arange(NPAN, dtype=jnp.int32)[:, None, None]
    panel_index = jnp.arange(NPAN, dtype=jnp.int32)[None, :, None]
    lower_part = slab_index > panel_index
    on_diagonal = slab_index == panel_index
    first_swapped = jnp.swapaxes(first, 0, 1)
    second_swapped = jnp.swapaxes(second, 0, 1)
    source_order = jnp.where(lower_part, second_swapped, first)
    target_order = jnp.where(lower_part, first_swapped, jnp.where(on_diagonal, first, second))
    target_inverse = jnp.argsort(target_order, axis=-1).astype(jnp.int32)
    extra_shifts = (jax.random.permutation(split_keys[1], ST // 2 - 1)[:(KP - 2) // 2] + 1).astype(jnp.int32)
    shifts = jnp.concatenate([jnp.array([0, ST // 2], jnp.int32), extra_shifts, -extra_shifts])
    position = (source_order[:, :, :, None] + shifts[None, None, None, :]) % ST
    columns = jnp.take_along_axis(target_inverse, position.reshape(NPAN, NPAN, ST * KP), axis=2)
    return jnp.transpose(columns.reshape(NPAN, NPAN, ST, KP), (0, 2, 1, 3)).astype(jnp.int32)


def draw_block_cols(key, part):
    return tile_pattern(key)


def draw_block_values(key, part):
    columns = tile_pattern(key)
    row_global = jnp.broadcast_to((jnp.arange(NPAN, dtype=jnp.int32)[:, None] * ST + jnp.arange(ST, dtype=jnp.int32)[None, :])[:, :, None, None], (NPAN, ST, NPAN, KP))
    col_global = jnp.arange(NPAN, dtype=jnp.int32)[None, None, :, None] * ST + columns
    tile_ident = (jnp.minimum(row_global, col_global) * NT + jnp.maximum(row_global, col_global)).reshape(-1)
    value_key = jax.random.fold_in(key, 23)

    def one_tile(ident):
        subkey = jax.random.fold_in(value_key, ident)
        return jax.random.normal(subkey, (TILE, TILE), jnp.float32)
    raw_tiles = jax.vmap(one_tile)(tile_ident)
    flipped = (row_global > col_global).reshape(-1)[:, None, None]
    diagonal_mask = (row_global == col_global).reshape(-1)[:, None, None]
    swapped = jnp.swapaxes(raw_tiles, 1, 2)
    tiles = jnp.where(flipped, swapped, raw_tiles)
    tiles = jnp.where(diagonal_mask, (raw_tiles + swapped) * 0.7071, tiles)
    scale = 2.0 / (NPAN * KP * TILE) ** 0.5
    return (tiles * scale).reshape(NPAN, ST, NPAN, KP, TILE, TILE).astype(jnp.bfloat16)


def setup_inputs(seed: int = 0) -> dict:
    splits = jax.random.split(jax.random.key(seed), 3)
    return {
        "block_values": draw_block_values(jax.random.fold_in(splits[2], 71), 0),
        "block_cols": draw_block_cols(jax.random.fold_in(splits[2], 71), 0),
    }


def dense_rows(row_tiles, row_columns):
    count_rows = row_tiles.shape[0]
    global_cols = (jnp.arange(NPAN, dtype=jnp.int32)[None, :, None] * ST + row_columns).reshape(count_rows, NPAN * KP)
    onehot = (global_cols[:, :, None] == jnp.arange(NT, dtype=jnp.int32)[None, None, :]).astype(jnp.float32)
    flattened = row_tiles.reshape(count_rows, NPAN * KP, TILE, TILE).astype(jnp.float32)
    densified = jnp.einsum("nqj,nqyx->nyjx", onehot, flattened)
    return densified.reshape(count_rows * TILE, ORDER)


def times_matrix(left_rows, block_values, block_cols):
    height = left_rows.shape[0]
    all_tiles = block_values.reshape(NT, NPAN * KP, TILE, TILE)
    all_columns = (jnp.arange(NPAN, dtype=jnp.int32)[None, :, None] * ST + block_cols.reshape(NT, NPAN, KP)).reshape(NT, NPAN * KP)

    def advance(running, inputs):
        row_tiles, row_columns, tile_row = inputs
        portion = lax.dynamic_slice_in_dim(left_rows, tile_row * TILE, TILE, 1)
        product = jnp.einsum("rx,qxy->rqy", portion, row_tiles.astype(jnp.float32))
        return running.at[:, row_columns, :].add(product), None

    running = jnp.zeros((height, NT, TILE), jnp.float32)
    running, ignored = lax.scan(advance, running, (all_tiles, all_columns, jnp.arange(NT, dtype=jnp.int32)))
    return running.reshape(height, ORDER)


def reference(block_values, block_cols):
    window_index = (jnp.arange(N_GX, dtype=jnp.int32)[:, None] * RB + jnp.arange(WIN, dtype=jnp.int32)[None, :]).reshape(-1)
    left_rows = dense_rows(block_values[0][window_index], block_cols[0][window_index])
    square = times_matrix(left_rows, block_values, block_cols)
    rounded = lax.optimization_barrier(square.astype(jnp.bfloat16)).astype(jnp.float32)
    return 3.0 * square - 2.0 * times_matrix(rounded, block_values, block_cols)
```

```python
import functools

import jax
import jax.numpy as jnp
from jax import lax
from jax.experimental import pallas as pl
from jax.experimental.pallas import tpu as pltpu
from jax.sharding import PartitionSpec as P

WIN = 1
LANES = 128
MESH = pl.DeviceIdType.MESH


def pieces_of(count, most):
    for pieces in range(min(count, most), 0, -1):
        if count % pieces == 0:
            return pieces


def greet(axes):
    barrier = pltpu.get_barrier_semaphore()
    total = 0
    for axis in axes:
        size = lax.axis_size(axis)
        me = lax.axis_index(axis)
        for step in range(1, size):
            pl.semaphore_signal(
                barrier, inc=1, device_id={axis: lax.rem(me + step, size)}, device_id_type=MESH
            )
        total += size - 1
    pl.semaphore_wait(barrier, total)


def remote(src, dst, send, recv, axis, peer):
    return pltpu.make_async_remote_copy(
        src_ref=src, dst_ref=dst, send_sem=send, recv_sem=recv,
        device_id={axis: peer}, device_id_type=MESH,
    )


def gather_kernel(
    n_gx, n_gy, pieces, tiles, cols, panel, panel_cols, left, left_cols,
    stage, load_sem, own_sem, send_sem, recv_sem, col_own, col_send, col_recv,
    win_own, win_send, win_recv,
):
    gx, gy = lax.axis_index("gx"), lax.axis_index("gy")
    rows = tiles.shape[0]
    part = rows // pieces
    loads = []
    for p in range(pieces):
        span = pl.ds(p * part, part)
        loads.append(pltpu.make_async_copy(tiles.at[span], stage.at[span], load_sem.at[p]))
        loads[-1].start()
    greet(("gx", "gy"))
    window = stage.at[pl.ds(0, WIN)]
    col_copies = [pltpu.make_async_copy(cols, panel_cols.at[gx], col_own)]
    for step in range(1, n_gx):
        col_copies.append(
            remote(cols, panel_cols.at[gx], col_send.at[step], col_recv.at[step],
                   "gx", lax.rem(gx + step, n_gx))
        )
    for copy in col_copies:
        copy.start()
    copies = []
    for p in range(pieces):
        loads[p].wait()
        if p == 0:
            @pl.when(gy == 0)
            def _():
                for peer in range(1, n_gy):
                    remote(window, left, win_send.at[0, peer], win_recv.at[0], "gy", peer).start()
                    remote(cols, left_cols, win_send.at[1, peer], win_recv.at[1], "gy", peer).start()
                pltpu.make_async_copy(window, left, win_own.at[0]).start()
                pltpu.make_async_copy(cols, left_cols, win_own.at[1]).start()
        source = stage.at[pl.ds(p * part, part)]
        target = panel.at[pl.ds(gx * rows + p * part, part)]
        for step in range(1, n_gx):
            copy = remote(source, target, send_sem.at[step, p], recv_sem.at[step, p],
                          "gx", lax.rem(gx + step, n_gx))
            copy.start()
            copies.append(copy)
        copy = pltpu.make_async_copy(source, target, own_sem.at[p])
        copy.start()
        copies.append(copy)
    for copy in col_copies + copies:
        copy.wait()

    @pl.when(gy == 0)
    def _():
        for peer in range(1, n_gy):
            remote(window, left, win_send.at[0, peer], win_recv.at[0], "gy", peer).wait_send()
            remote(cols, left_cols, win_send.at[1, peer], win_recv.at[1], "gy", peer).wait_send()
        pltpu.make_async_copy(window, left, win_own.at[0]).wait()
        pltpu.make_async_copy(cols, left_cols, win_own.at[1]).wait()

    @pl.when(gy != 0)
    def _():
        remote(window, left, win_send.at[0, 0], win_recv.at[0], "gy", 0).wait_recv()
        remote(cols, left_cols, win_send.at[1, 0], win_recv.at[1], "gy", 0).wait_recv()


def gather(tiles, cols):
    n_gx, n_gy = lax.axis_size("gx"), lax.axis_size("gy")
    rows = tiles.shape[0]
    pieces = pieces_of(rows, 4)
    padded = jnp.pad(cols, ((0, 0), (0, LANES - cols.shape[1])))
    dma = pltpu.SemaphoreType.DMA
    return pl.pallas_call(
        functools.partial(gather_kernel, n_gx, n_gy, pieces),
        out_shape=(
            jax.ShapeDtypeStruct((n_gx * rows,) + tiles.shape[1:], tiles.dtype),
            jax.ShapeDtypeStruct((n_gx,) + padded.shape, padded.dtype),
            jax.ShapeDtypeStruct((WIN,) + tiles.shape[1:], tiles.dtype),
            jax.ShapeDtypeStruct(padded.shape, padded.dtype),
        ),
        in_specs=[
            pl.BlockSpec(memory_space=pl.ANY),
            pl.BlockSpec(memory_space=pltpu.VMEM),
        ],
        out_specs=[pl.BlockSpec(memory_space=pl.ANY)] * 4,
        scratch_shapes=[
            pltpu.VMEM(tiles.shape, tiles.dtype),
            dma((pieces,)), dma((pieces,)), dma((n_gx, pieces)), dma((n_gx, pieces)),
            dma, dma((n_gx,)), dma((n_gx,)),
            dma((2,)), dma((2, n_gy)), dma((2,)),
        ],
        compiler_params=pltpu.CompilerParams(collective_id=0, has_side_effects=True),
        name="gather_tiles",
    )(tiles, padded)


def first_kernel(block, slots, left_cols, panel_cols, left, tiles, out, dense):
    step = pl.program_id(0)

    @pl.when(step == 0)
    def _():
        dense[...] = jnp.zeros_like(dense)
        for k in range(slots):
            dense[left_cols[k]] = left[k]

    for r in range(block):
        base = (step * block + r) * slots
        picked = jnp.concatenate([dense[panel_cols[base + k]] for k in range(slots)], axis=1)
        held = jnp.concatenate([tiles[r, k] for k in range(slots)], axis=1)
        product = lax.dot_general(
            picked, held, (((1,), (1,)), ((), ())), preferred_element_type=jnp.float32
        )
        out[r] = product.astype(out.dtype)


def first(left, left_cols, panel, panel_cols):
    count, slots, size = panel.shape[0], panel.shape[1], panel.shape[2]
    block = pieces_of(count, 8)
    return pl.pallas_call(
        functools.partial(first_kernel, block, slots),
        out_shape=jax.ShapeDtypeStruct((count, size, size), panel.dtype),
        grid=(count // block,),
        in_specs=[
            pl.BlockSpec(memory_space=pltpu.SMEM),
            pl.BlockSpec(memory_space=pltpu.SMEM),
            pl.BlockSpec(left.shape, lambda i: (0, 0, 0)),
            pl.BlockSpec((block, slots, size, size), lambda i: (i, 0, 0, 0)),
        ],
        out_specs=pl.BlockSpec((block, size, size), lambda i: (i, 0, 0)),
        scratch_shapes=[pltpu.VMEM((count, size, size), panel.dtype)],
        compiler_params=pltpu.CompilerParams(dimension_semantics=("arbitrary",)),
        name="square_partial",
    )(left_cols, panel_cols, left, panel)


def reduce_kernel(size, pieces, part, own, out, landed, send_a, recv_a, send_b, recv_b):
    me = lax.axis_index("gz")
    step_rows = part.shape[0] // size
    rows = step_rows // pieces
    greet(("gz",))
    scatters, gathers = [], []
    for p in range(pieces):
        for d in range(1, size):
            peer = lax.rem(me + d, size)
            copy = remote(
                part.at[pl.ds(peer * step_rows + p * rows, rows)], landed.at[d - 1, p],
                send_a.at[d - 1, p], recv_a.at[d - 1, p], "gz", peer,
            )
            copy.start()
            scatters.append(copy)
    for p in range(pieces):
        for d in range(1, size):
            scatters[p * (size - 1) + d - 1].wait_recv()
        start = me * step_rows + p * rows
        for r in range(rows):
            total = part[start + r].astype(jnp.float32)
            for d in range(1, size):
                total = total + landed[d - 1, p, r].astype(jnp.float32)
            out[start + r] = total.astype(out.dtype)
        span = pl.ds(start, rows)
        for d in range(1, size):
            copy = remote(
                out.at[span], out.at[span],
                send_b.at[d - 1, p], recv_b.at[d - 1, p], "gz", lax.rem(me + d, size),
            )
            copy.start()
            gathers.append(copy)
    for copy in scatters:
        copy.wait_send()
    for copy in gathers:
        copy.wait()


def reduce_square(part):
    size = lax.axis_size("gz")
    step_rows = part.shape[0] // size
    pieces = pieces_of(step_rows, 4)
    dma = pltpu.SemaphoreType.DMA
    landed = (size - 1, pieces, step_rows // pieces) + part.shape[1:]

    def body(part_ref, out, landed_ref, *sems):
        reduce_kernel(size, pieces, part_ref, None, out, landed_ref, *sems)

    return pl.pallas_call(
        body,
        out_shape=jax.ShapeDtypeStruct(part.shape, part.dtype),
        in_specs=[pl.BlockSpec(memory_space=pltpu.VMEM)],
        out_specs=pl.BlockSpec(memory_space=pltpu.VMEM),
        scratch_shapes=[pltpu.VMEM(landed, part.dtype)] + [dma((size - 1, pieces))] * 4,
        compiler_params=pltpu.CompilerParams(collective_id=1, has_side_effects=True),
        name="square_reduce",
    )(part)


def second_kernel(block, slots, groups, panel_cols, square, tiles, out, total):
    step = pl.program_id(0)
    count = total.shape[0]
    height = total.shape[1] // groups

    @pl.when(step == 0)
    def _():
        total[...] = jnp.zeros_like(total)

    for r in range(block):
        row = step * block + r
        base = row * slots
        for k in range(0, slots, 2):
            held = jnp.concatenate([tiles[r, j] for j in range(k, min(k + 2, slots))], axis=1)
            product = jnp.dot(square[row], held, preferred_element_type=jnp.float32)
            for j in range(k, min(k + 2, slots)):
                width = tiles.shape[3]
                total[panel_cols[base + j]] += product[:, (j - k) * width:(j - k + 1) * width]

    @pl.when(step == pl.num_programs(0) - 1)
    def _():
        same = (lax.axis_index("gy") == lax.axis_index("gz")).astype(jnp.float32)

        @pl.loop(0, count)
        def _(c):
            value = (3.0 * same) * square[c].astype(jnp.float32) - 2.0 * total[c]
            value = value.astype(out.dtype)
            for g in range(groups):
                out[g, c] = value[g * height:(g + 1) * height]


def second(square, panel, panel_cols):
    count, slots, size = panel.shape[0], panel.shape[1], panel.shape[2]
    groups = lax.axis_size("gy")
    block = pieces_of(count, 8)
    shape = (groups, count, size // groups, size)
    return pl.pallas_call(
        functools.partial(second_kernel, block, slots, groups),
        out_shape=jax.ShapeDtypeStruct(shape, panel.dtype),
        grid=(count // block,),
        in_specs=[
            pl.BlockSpec(memory_space=pltpu.SMEM),
            pl.BlockSpec(square.shape, lambda i: (0, 0, 0)),
            pl.BlockSpec((block, slots, size, size), lambda i: (i, 0, 0, 0)),
        ],
        out_specs=pl.BlockSpec(shape, lambda i: (0, 0, 0, 0)),
        scratch_shapes=[pltpu.VMEM((count, size, size), jnp.float32)],
        compiler_params=pltpu.CompilerParams(dimension_semantics=("arbitrary",)),
        name="cube_partial",
    )(panel_cols, square, panel)


def scatter_kernel(size, pieces, part, out, landed, send, recv):
    me = lax.axis_index("gy")
    rows = part.shape[1] // pieces
    width = part.shape[3]
    greet(("gy",))
    copies = []
    for p in range(pieces):
        span = pl.ds(p * rows, rows)
        for d in range(1, size):
            peer = lax.rem(me + d, size)
            copy = remote(part.at[peer, span], landed.at[d - 1, p],
                          send.at[d - 1, p], recv.at[d - 1, p], "gy", peer)
            copy.start()
            copies.append(copy)
    for p in range(pieces):
        for d in range(1, size):
            copies[p * (size - 1) + d - 1].wait_recv()
        for r in range(rows):
            c = p * rows + r
            total = part[me, c].astype(jnp.float32)
            for d in range(1, size):
                total = total + landed[d - 1, p, r].astype(jnp.float32)
            out[:, c * width:(c + 1) * width] = total
    for copy in copies:
        copy.wait_send()


def scatter_result(part):
    size = lax.axis_size("gy")
    count, height, width = part.shape[1:]
    pieces = pieces_of(count, 4)
    dma = pltpu.SemaphoreType.DMA
    return pl.pallas_call(
        functools.partial(scatter_kernel, size, pieces),
        out_shape=jax.ShapeDtypeStruct((height, count * width), jnp.float32),
        in_specs=[pl.BlockSpec(memory_space=pltpu.VMEM)],
        out_specs=pl.BlockSpec(memory_space=pltpu.VMEM),
        scratch_shapes=[
            pltpu.VMEM((size - 1, pieces, count // pieces, height, width), part.dtype),
            dma((size - 1, pieces)), dma((size - 1, pieces)),
        ],
        compiler_params=pltpu.CompilerParams(collective_id=2, has_side_effects=True),
        name="result_scatter",
    )(part)


def local(block_values, block_cols):
    tiles = block_values[0, :, 0]
    cols = block_cols[0, :, 0]
    slots = cols.shape[1]
    panel, panel_cols, left, left_cols = gather(tiles, cols)
    panel_cols = panel_cols[:, :, :slots].reshape(-1)
    left_cols = left_cols[0, :slots]
    part = first(left[0], left_cols, panel, panel_cols)
    square = reduce_square(part)
    return scatter_result(second(square, panel, panel_cols))


def solution(mesh):
    in_specs = (P("gy", "gx", "gz", None, None, None), P("gy", "gx", "gz", None))
    out_specs = P(("gx", "gy"), "gz")
    return jax.shard_map(local, mesh=mesh, in_specs=in_specs, out_specs=out_specs, check_vma=False)
```

```python
import functools

import jax
import jax.numpy as jnp
from jax import lax
from jax.experimental import pallas as pl
from jax.experimental.pallas import tpu as pltpu
from jax.sharding import PartitionSpec as P

WIN = 1
LANES = 128
MESH = pl.DeviceIdType.MESH


def pieces_of(count, most):
    for pieces in range(min(count, most), 0, -1):
        if count % pieces == 0:
            return pieces


def greet(axes):
    barrier = pltpu.get_barrier_semaphore()
    total = 0
    for axis in axes:
        size = lax.axis_size(axis)
        me = lax.axis_index(axis)
        for step in range(1, size):
            pl.semaphore_signal(
                barrier, inc=1, device_id={axis: lax.rem(me + step, size)}, device_id_type=MESH
            )
        total += size - 1
    pl.semaphore_wait(barrier, total)


def remote(src, dst, send, recv, axis, peer):
    return pltpu.make_async_remote_copy(
        src_ref=src, dst_ref=dst, send_sem=send, recv_sem=recv,
        device_id={axis: peer}, device_id_type=MESH,
    )


def gather_kernel(
    n_gx, n_gy, pieces, tiles, cols, panel, panel_cols, left, left_cols,
    stage, load_sem, own_sem, send_sem, recv_sem, col_own, col_send, col_recv,
    win_own, win_send, win_recv,
):
    gx, gy = lax.axis_index("gx"), lax.axis_index("gy")
    rows = tiles.shape[0]
    part = rows // pieces
    loads = []
    for p in range(pieces):
        span = pl.ds(p * part, part)
        loads.append(pltpu.make_async_copy(tiles.at[span], stage.at[span], load_sem.at[p]))
        loads[-1].start()
    greet(("gx", "gy"))
    window = stage.at[pl.ds(0, WIN)]
    col_copies = [pltpu.make_async_copy(cols, panel_cols.at[gx], col_own)]
    for step in range(1, n_gx):
        col_copies.append(
            remote(cols, panel_cols.at[gx], col_send.at[step], col_recv.at[step],
                   "gx", lax.rem(gx + step, n_gx))
        )
    for copy in col_copies:
        copy.start()
    copies = []
    for p in range(pieces):
        loads[p].wait()
        if p == 0:
            @pl.when(gy == 0)
            def _():
                for peer in range(1, n_gy):
                    remote(window, left, win_send.at[0, peer], win_recv.at[0], "gy", peer).start()
                    remote(cols, left_cols, win_send.at[1, peer], win_recv.at[1], "gy", peer).start()
                pltpu.make_async_copy(window, left, win_own.at[0]).start()
                pltpu.make_async_copy(cols, left_cols, win_own.at[1]).start()
        source = stage.at[pl.ds(p * part, part)]
        target = panel.at[pl.ds(gx * rows + p * part, part)]
        for step in range(1, n_gx):
            copy = remote(source, target, send_sem.at[step, p], recv_sem.at[step, p],
                          "gx", lax.rem(gx + step, n_gx))
            copy.start()
            copies.append(copy)
        copy = pltpu.make_async_copy(source, target, own_sem.at[p])
        copy.start()
        copies.append(copy)
    for copy in col_copies + copies:
        copy.wait()

    @pl.when(gy == 0)
    def _():
        for peer in range(1, n_gy):
            remote(window, left, win_send.at[0, peer], win_recv.at[0], "gy", peer).wait_send()
            remote(cols, left_cols, win_send.at[1, peer], win_recv.at[1], "gy", peer).wait_send()
        pltpu.make_async_copy(window, left, win_own.at[0]).wait()
        pltpu.make_async_copy(cols, left_cols, win_own.at[1]).wait()

    @pl.when(gy != 0)
    def _():
        remote(window, left, win_send.at[0, 0], win_recv.at[0], "gy", 0).wait_recv()
        remote(cols, left_cols, win_send.at[1, 0], win_recv.at[1], "gy", 0).wait_recv()


def gather(tiles, cols):
    n_gx, n_gy = lax.axis_size("gx"), lax.axis_size("gy")
    rows = tiles.shape[0]
    pieces = pieces_of(rows, 4)
    padded = jnp.pad(cols, ((0, 0), (0, LANES - cols.shape[1])))
    dma = pltpu.SemaphoreType.DMA
    return pl.pallas_call(
        functools.partial(gather_kernel, n_gx, n_gy, pieces),
        out_shape=(
            jax.ShapeDtypeStruct((n_gx * rows,) + tiles.shape[1:], tiles.dtype),
            jax.ShapeDtypeStruct((n_gx,) + padded.shape, padded.dtype),
            jax.ShapeDtypeStruct((WIN,) + tiles.shape[1:], tiles.dtype),
            jax.ShapeDtypeStruct(padded.shape, padded.dtype),
        ),
        in_specs=[
            pl.BlockSpec(memory_space=pl.ANY),
            pl.BlockSpec(memory_space=pltpu.VMEM),
        ],
        out_specs=[pl.BlockSpec(memory_space=pl.ANY)] * 4,
        scratch_shapes=[
            pltpu.VMEM(tiles.shape, tiles.dtype),
            dma((pieces,)), dma((pieces,)), dma((n_gx, pieces)), dma((n_gx, pieces)),
            dma, dma((n_gx,)), dma((n_gx,)),
            dma((2,)), dma((2, n_gy)), dma((2,)),
        ],
        compiler_params=pltpu.CompilerParams(collective_id=0, has_side_effects=True),
        name="gather_tiles",
    )(tiles, padded)


def first_kernel(
    slots, pairs, left_cols, panel_cols, left, panel, out, rows_out,
    inverse, place, which, stage, sem,
):
    groups, height = out.shape[0], out.shape[2]

    @pl.loop(0, inverse.shape[0])
    def _(c):
        inverse[c] = -1

    @pl.loop(0, rows_out.shape[1])
    def _(c):
        rows_out[0, c] = 0

    for k in range(slots):
        inverse[left_cols[k]] = k

    def scan(entry, found):
        k = inverse[panel_cols[entry]]
        place[found] = entry
        which[found] = k
        return found + (k >= 0).astype(jnp.int32)

    lax.fori_loop(0, panel.shape[0], scan, jnp.int32(0), unroll=8)
    copies = []
    for n in range(pairs):
        copies.append(pltpu.make_async_copy(panel.at[place[n]], stage.at[n], sem.at[n]))
        copies[-1].start()
    for n in range(pairs):
        rows_out[0, n] = lax.div(place[n], jnp.int32(slots))
        copies[n].wait()
        product = lax.dot_general(
            left[which[n]], stage[n], (((1,), (1,)), ((), ())),
            preferred_element_type=jnp.float32,
        ).astype(out.dtype)
        for g in range(groups):
            out[g, n] = product[g * height:(g + 1) * height]


def first(left, left_cols, panel, panel_cols):
    count, slots, size = panel.shape[0], panel.shape[1], panel.shape[2]
    pairs = slots * slots
    groups = lax.axis_size("gz")
    smem = pl.BlockSpec(memory_space=pltpu.SMEM)
    vmem = pl.BlockSpec(memory_space=pltpu.VMEM)
    return pl.pallas_call(
        functools.partial(first_kernel, slots, pairs),
        out_shape=(
            jax.ShapeDtypeStruct((groups, pairs, size // groups, size), panel.dtype),
            jax.ShapeDtypeStruct((1, LANES), jnp.int32),
        ),
        in_specs=[smem, smem, vmem, pl.BlockSpec(memory_space=pl.ANY)],
        out_specs=(vmem, smem),
        scratch_shapes=[
            pltpu.SMEM((count,), jnp.int32),
            pltpu.SMEM((pairs + 1,), jnp.int32),
            pltpu.SMEM((pairs + 1,), jnp.int32),
            pltpu.VMEM((pairs, size, size), panel.dtype),
            pltpu.SemaphoreType.DMA((pairs,)),
        ],
        name="square_products",
    )(left_cols, panel_cols, left, panel.reshape(count * slots, size, size))


def exchange_kernel(size, part, rows, landed, rows_landed, own, send, recv, row_send, row_recv):
    me = lax.axis_index("gz")
    greet(("gz",))
    copies = [
        pltpu.make_async_copy(part.at[me], landed.at[me], own.at[0]),
        pltpu.make_async_copy(rows, rows_landed.at[me], own.at[1]),
    ]
    for d in range(1, size):
        peer = lax.rem(me + d, size)
        copies.append(remote(part.at[peer], landed.at[me], send.at[d - 1], recv.at[d - 1], "gz", peer))
        copies.append(
            remote(rows, rows_landed.at[me], row_send.at[d - 1], row_recv.at[d - 1], "gz", peer)
        )
    for copy in copies:
        copy.start()
    for copy in copies:
        copy.wait()


def exchange(part, rows):
    size = lax.axis_size("gz")
    dma = pltpu.SemaphoreType.DMA
    vmem = pl.BlockSpec(memory_space=pltpu.VMEM)
    return pl.pallas_call(
        functools.partial(exchange_kernel, size),
        out_shape=(
            jax.ShapeDtypeStruct(part.shape, part.dtype),
            jax.ShapeDtypeStruct((size,) + rows.shape, rows.dtype),
        ),
        in_specs=[vmem, vmem],
        out_specs=(vmem, vmem),
        scratch_shapes=[dma((2,))] + [dma((size - 1,))] * 4,
        compiler_params=pltpu.CompilerParams(collective_id=1, has_side_effects=True),
        name="square_exchange",
    )(part, rows)


def sum_kernel(rows, landed, out, total):
    total[...] = jnp.zeros_like(total)
    for b in range(landed.shape[0]):
        for n in range(landed.shape[1]):
            total[rows[b, 0, n]] += landed[b, n].astype(jnp.float32)
    out[...] = total[...].astype(out.dtype)


def sum_products(landed, rows, count):
    shape = (count,) + landed.shape[2:]
    vmem = pl.BlockSpec(memory_space=pltpu.VMEM)
    return pl.pallas_call(
        sum_kernel,
        out_shape=jax.ShapeDtypeStruct(shape, landed.dtype),
        in_specs=[pl.BlockSpec(memory_space=pltpu.SMEM), vmem],
        out_specs=vmem,
        scratch_shapes=[pltpu.VMEM(shape, jnp.float32)],
        name="square_sum",
    )(rows, landed)


def spread_kernel(size, pieces, chunk, out, own, send, recv):
    me = lax.axis_index("gz")
    rows = chunk.shape[0] // pieces
    greet(("gz",))
    keep = pltpu.make_async_copy(chunk, out.at[me], own)
    keep.start()

    def hop(side, step, p):
        way = 1 - 2 * side
        block = me - way * step
        span = pl.ds(p * rows, rows)
        source = chunk.at[span] if step == 0 else out.at[block, span]
        copy = remote(source, out.at[block, span], send.at[side, step, p], recv.at[side, step, p],
                      "gz", lax.rem(me + way + size, size))
        ahead = me + way
        valid = (block >= 0) & (block < size) & (ahead >= 0) & (ahead < size)
        return copy, valid

    def landing(side, step, p):
        way = 1 - 2 * side
        block = me - way * (step + 1)
        span = pl.ds(p * rows, rows)
        copy = remote(out.at[block, span], out.at[block, span], send.at[side, step, p],
                      recv.at[side, step, p], "gz", lax.rem(me + way + size, size))
        return copy, (block >= 0) & (block < size)

    def send_hop(side, step, p):
        copy, valid = hop(side, step, p)

        @pl.when(valid)
        def _():
            copy.start()

    for p in range(pieces):
        for side in range(2):
            send_hop(side, 0, p)
    for step in range(size - 1):
        for p in range(pieces):
            for side in range(2):
                copy, valid = landing(side, step, p)

                @pl.when(valid)
                def _():
                    copy.wait_recv()

                if step + 1 < size - 1:
                    send_hop(side, step + 1, p)
    for step in range(size - 1):
        for p in range(pieces):
            for side in range(2):
                copy, valid = hop(side, step, p)

                @pl.when(valid)
                def _():
                    copy.wait_send()
    keep.wait()


def spread(chunk):
    size = lax.axis_size("gz")
    pieces = pieces_of(chunk.shape[0], 4)
    dma = pltpu.SemaphoreType.DMA
    vmem = pl.BlockSpec(memory_space=pltpu.VMEM)
    return pl.pallas_call(
        functools.partial(spread_kernel, size, pieces),
        out_shape=jax.ShapeDtypeStruct((size,) + chunk.shape, chunk.dtype),
        in_specs=[vmem],
        out_specs=vmem,
        scratch_shapes=[dma, dma((2, size - 1, pieces)), dma((2, size - 1, pieces))],
        compiler_params=pltpu.CompilerParams(collective_id=3, has_side_effects=True),
        name="square_spread",
    )(chunk)


def second_kernel(block, slots, groups, panel_cols, square, tiles, out, total):
    step = pl.program_id(0)
    count = total.shape[0]
    height = total.shape[1] // groups

    def rows_of(c):
        return jnp.concatenate([square[q, c] for q in range(square.shape[0])], axis=0)

    @pl.when(step == 0)
    def _():
        total[...] = jnp.zeros_like(total)

    for r in range(block):
        row = step * block + r
        base = row * slots
        rounded = rows_of(row)
        for k in range(0, slots, 2):
            held = jnp.concatenate([tiles[r, j] for j in range(k, min(k + 2, slots))], axis=1)
            product = jnp.dot(rounded, held, preferred_element_type=jnp.float32)
            for j in range(k, min(k + 2, slots)):
                width = tiles.shape[3]
                total[panel_cols[base + j]] += product[:, (j - k) * width:(j - k + 1) * width]

    @pl.when(step == pl.num_programs(0) - 1)
    def _():
        same = (lax.axis_index("gy") == lax.axis_index("gz")).astype(jnp.float32)

        @pl.loop(0, count)
        def _(c):
            value = (3.0 * same) * rows_of(c).astype(jnp.float32) - 2.0 * total[c]
            value = value.astype(out.dtype)
            for g in range(groups):
                out[g, c] = value[g * height:(g + 1) * height]


def second(square, panel, panel_cols):
    count, slots, size = panel.shape[0], panel.shape[1], panel.shape[2]
    groups = lax.axis_size("gy")
    block = pieces_of(count, 8)
    shape = (groups, count, size // groups, size)
    return pl.pallas_call(
        functools.partial(second_kernel, block, slots, groups),
        out_shape=jax.ShapeDtypeStruct(shape, panel.dtype),
        grid=(count // block,),
        in_specs=[
            pl.BlockSpec(memory_space=pltpu.SMEM),
            pl.BlockSpec(square.shape, lambda i: (0, 0, 0, 0)),
            pl.BlockSpec((block, slots, size, size), lambda i: (i, 0, 0, 0)),
        ],
        out_specs=pl.BlockSpec(shape, lambda i: (0, 0, 0, 0)),
        scratch_shapes=[pltpu.VMEM((count, size, size), jnp.float32)],
        compiler_params=pltpu.CompilerParams(dimension_semantics=("arbitrary",)),
        name="cube_partial",
    )(panel_cols, square, panel)


def scatter_kernel(size, pieces, part, out, landed, send, recv):
    me = lax.axis_index("gy")
    rows = part.shape[1] // pieces
    width = part.shape[3]
    greet(("gy",))
    copies = []
    for p in range(pieces):
        span = pl.ds(p * rows, rows)
        for d in range(1, size):
            peer = lax.rem(me + d, size)
            copy = remote(part.at[peer, span], landed.at[d - 1, p],
                          send.at[d - 1, p], recv.at[d - 1, p], "gy", peer)
            copy.start()
            copies.append(copy)
    for p in range(pieces):
        for d in range(1, size):
            copies[p * (size - 1) + d - 1].wait_recv()
        for r in range(rows):
            c = p * rows + r
            total = part[me, c].astype(jnp.float32)
            for d in range(1, size):
                total = total + landed[d - 1, p, r].astype(jnp.float32)
            out[:, c * width:(c + 1) * width] = total
    for copy in copies:
        copy.wait_send()


def scatter_result(part):
    size = lax.axis_size("gy")
    count, height, width = part.shape[1:]
    pieces = pieces_of(count, 4)
    dma = pltpu.SemaphoreType.DMA
    return pl.pallas_call(
        functools.partial(scatter_kernel, size, pieces),
        out_shape=jax.ShapeDtypeStruct((height, count * width), jnp.float32),
        in_specs=[pl.BlockSpec(memory_space=pltpu.VMEM)],
        out_specs=pl.BlockSpec(memory_space=pltpu.VMEM),
        scratch_shapes=[
            pltpu.VMEM((size - 1, pieces, count // pieces, height, width), part.dtype),
            dma((size - 1, pieces)), dma((size - 1, pieces)),
        ],
        compiler_params=pltpu.CompilerParams(collective_id=2, has_side_effects=True),
        name="result_scatter",
    )(part)


def local(block_values, block_cols):
    tiles = block_values[0, :, 0]
    cols = block_cols[0, :, 0]
    slots = cols.shape[1]
    panel, panel_cols, left, left_cols = gather(tiles, cols)
    panel_cols = panel_cols[:, :, :slots].reshape(-1)
    left_cols = left_cols[0, :slots]
    part, rows = first(left[0], left_cols, panel, panel_cols)
    landed, rows = exchange(part, rows)
    square = spread(sum_products(landed, rows, panel.shape[0]))
    return scatter_result(second(square, panel, panel_cols))


def solution(mesh):
    in_specs = (P("gy", "gx", "gz", None, None, None), P("gy", "gx", "gz", None))
    out_specs = P(("gx", "gy"), "gz")
    return jax.shard_map(local, mesh=mesh, in_specs=in_specs, out_specs=out_specs, check_vma=False)
```

```python
import functools

import jax
import jax.numpy as jnp
from jax import lax
from jax.experimental import pallas as pl
from jax.experimental.pallas import tpu as pltpu
from jax.sharding import PartitionSpec as P

WIN = 1
LANES = 128
MESH = pl.DeviceIdType.MESH


def pieces_of(count, most):
    for pieces in range(min(count, most), 0, -1):
        if count % pieces == 0:
            return pieces


def greet(axes):
    barrier = pltpu.get_barrier_semaphore()
    total = 0
    for axis in axes:
        size = lax.axis_size(axis)
        me = lax.axis_index(axis)
        for step in range(1, size):
            pl.semaphore_signal(
                barrier, inc=1, device_id={axis: lax.rem(me + step, size)}, device_id_type=MESH
            )
        total += size - 1
    pl.semaphore_wait(barrier, total)


def remote(src, dst, send, recv, axis, peer):
    return pltpu.make_async_remote_copy(
        src_ref=src, dst_ref=dst, send_sem=send, recv_sem=recv,
        device_id={axis: peer}, device_id_type=MESH,
    )


def gather_kernel(
    n_gx, n_gy, pieces, tiles, cols, panel, panel_cols, left, left_cols,
    stage, load_sem, own_sem, send_sem, recv_sem, col_own, col_send, col_recv,
    win_own, win_send, win_recv,
):
    gx, gy = lax.axis_index("gx"), lax.axis_index("gy")
    rows = tiles.shape[0]
    part = rows // pieces
    loads = []
    for p in range(pieces):
        span = pl.ds(p * part, part)
        loads.append(pltpu.make_async_copy(tiles.at[span], stage.at[span], load_sem.at[p]))
        loads[-1].start()
    greet(("gx", "gy"))
    window = stage.at[pl.ds(0, WIN)]
    col_copies = [pltpu.make_async_copy(cols, panel_cols.at[gx], col_own)]
    for step in range(1, n_gx):
        col_copies.append(
            remote(cols, panel_cols.at[gx], col_send.at[step], col_recv.at[step],
                   "gx", lax.rem(gx + step, n_gx))
        )
    for copy in col_copies:
        copy.start()
    copies = []
    for p in range(pieces):
        loads[p].wait()
        if p == 0:
            @pl.when(gy == 0)
            def _():
                for peer in range(1, n_gy):
                    remote(window, left, win_send.at[0, peer], win_recv.at[0], "gy", peer).start()
                    remote(cols, left_cols, win_send.at[1, peer], win_recv.at[1], "gy", peer).start()
                pltpu.make_async_copy(window, left, win_own.at[0]).start()
                pltpu.make_async_copy(cols, left_cols, win_own.at[1]).start()
        source = stage.at[pl.ds(p * part, part)]
        target = panel.at[pl.ds(gx * rows + p * part, part)]
        for step in range(1, n_gx):
            copy = remote(source, target, send_sem.at[step, p], recv_sem.at[step, p],
                          "gx", lax.rem(gx + step, n_gx))
            copy.start()
            copies.append(copy)
        copy = pltpu.make_async_copy(source, target, own_sem.at[p])
        copy.start()
        copies.append(copy)
    for copy in col_copies + copies:
        copy.wait()

    @pl.when(gy == 0)
    def _():
        for peer in range(1, n_gy):
            remote(window, left, win_send.at[0, peer], win_recv.at[0], "gy", peer).wait_send()
            remote(cols, left_cols, win_send.at[1, peer], win_recv.at[1], "gy", peer).wait_send()
        pltpu.make_async_copy(window, left, win_own.at[0]).wait()
        pltpu.make_async_copy(cols, left_cols, win_own.at[1]).wait()

    @pl.when(gy != 0)
    def _():
        remote(window, left, win_send.at[0, 0], win_recv.at[0], "gy", 0).wait_recv()
        remote(cols, left_cols, win_send.at[1, 0], win_recv.at[1], "gy", 0).wait_recv()


def gather(tiles, cols):
    n_gx, n_gy = lax.axis_size("gx"), lax.axis_size("gy")
    rows = tiles.shape[0]
    pieces = pieces_of(rows, 4)
    padded = jnp.pad(cols, ((0, 0), (0, LANES - cols.shape[1])))
    dma = pltpu.SemaphoreType.DMA
    return pl.pallas_call(
        functools.partial(gather_kernel, n_gx, n_gy, pieces),
        out_shape=(
            jax.ShapeDtypeStruct((n_gx * rows,) + tiles.shape[1:], tiles.dtype),
            jax.ShapeDtypeStruct((n_gx,) + padded.shape, padded.dtype),
            jax.ShapeDtypeStruct((WIN,) + tiles.shape[1:], tiles.dtype),
            jax.ShapeDtypeStruct(padded.shape, padded.dtype),
        ),
        in_specs=[
            pl.BlockSpec(memory_space=pl.ANY),
            pl.BlockSpec(memory_space=pltpu.VMEM),
        ],
        out_specs=[pl.BlockSpec(memory_space=pl.ANY)] * 4,
        scratch_shapes=[
            pltpu.VMEM(tiles.shape, tiles.dtype),
            dma((pieces,)), dma((pieces,)), dma((n_gx, pieces)), dma((n_gx, pieces)),
            dma, dma((n_gx,)), dma((n_gx,)),
            dma((2,)), dma((2, n_gy)), dma((2,)),
        ],
        compiler_params=pltpu.CompilerParams(collective_id=0, has_side_effects=True),
        name="gather_tiles",
    )(tiles, padded)


def first_kernel(
    slots, pairs, left_cols, panel_cols, left, panel, out, rows_out,
    inverse, place, which, stage, sem,
):
    groups, height = out.shape[0], out.shape[2]

    for c in range(inverse.shape[0]):
        inverse[c] = -1
    for c in range(pairs, rows_out.shape[1]):
        rows_out[0, c] = 0
    for k in range(slots):
        inverse[left_cols[k]] = k
    entries = panel.shape[0]
    group = pieces_of(entries, 32)

    def scan(step, found):
        base = step * group
        matches = [inverse[panel_cols[base + j]] for j in range(group)]
        for j, k in enumerate(matches):
            place[found] = base + j
            which[found] = k
            found = found + (k >= 0).astype(jnp.int32)
        return found

    lax.fori_loop(0, entries // group, scan, jnp.int32(0))
    bunch = pairs // pieces_of(pairs, 4)
    copies = []
    for n in range(pairs):
        copies.append(pltpu.make_async_copy(panel.at[place[n]], stage.at[n], sem.at[n]))
        copies[-1].start()
    for n in range(pairs):
        rows_out[0, n] = lax.div(place[n], jnp.int32(slots))
    for first_pair in range(0, pairs, bunch):
        span = range(first_pair, first_pair + bunch)
        for n in span:
            copies[n].wait()
        for n in span:
            product = lax.dot_general(
                left[which[n]], stage[n], (((1,), (1,)), ((), ())),
                preferred_element_type=jnp.float32,
            ).astype(out.dtype)
            for g in range(groups):
                out[g, n] = product[g * height:(g + 1) * height]


def first(left, left_cols, panel, panel_cols):
    count, slots, size = panel.shape[0], panel.shape[1], panel.shape[2]
    pairs = slots * slots
    groups = lax.axis_size("gz")
    smem = pl.BlockSpec(memory_space=pltpu.SMEM)
    vmem = pl.BlockSpec(memory_space=pltpu.VMEM)
    return pl.pallas_call(
        functools.partial(first_kernel, slots, pairs),
        out_shape=(
            jax.ShapeDtypeStruct((groups, pairs, size // groups, size), panel.dtype),
            jax.ShapeDtypeStruct((1, LANES), jnp.int32),
        ),
        in_specs=[smem, smem, vmem, pl.BlockSpec(memory_space=pl.ANY)],
        out_specs=(vmem, smem),
        scratch_shapes=[
            pltpu.SMEM((count,), jnp.int32),
            pltpu.SMEM((pairs + 1,), jnp.int32),
            pltpu.SMEM((pairs + 1,), jnp.int32),
            pltpu.VMEM((pairs, size, size), panel.dtype),
            pltpu.SemaphoreType.DMA((pairs,)),
        ],
        name="square_products",
    )(left_cols, panel_cols, left, panel.reshape(count * slots, size, size))


def exchange_kernel(size, part, rows, landed, rows_landed, own, send, recv, row_send, row_recv):
    me = lax.axis_index("gz")
    greet(("gz",))
    copies = [
        pltpu.make_async_copy(part.at[me], landed.at[me], own.at[0]),
        pltpu.make_async_copy(rows, rows_landed.at[me], own.at[1]),
    ]
    for d in range(1, size):
        peer = lax.rem(me + d, size)
        copies.append(remote(part.at[peer], landed.at[me], send.at[d - 1], recv.at[d - 1], "gz", peer))
        copies.append(
            remote(rows, rows_landed.at[me], row_send.at[d - 1], row_recv.at[d - 1], "gz", peer)
        )
    for copy in copies:
        copy.start()
    for copy in copies:
        copy.wait()


def exchange(part, rows):
    size = lax.axis_size("gz")
    dma = pltpu.SemaphoreType.DMA
    vmem = pl.BlockSpec(memory_space=pltpu.VMEM)
    return pl.pallas_call(
        functools.partial(exchange_kernel, size),
        out_shape=(
            jax.ShapeDtypeStruct(part.shape, part.dtype),
            jax.ShapeDtypeStruct((size,) + rows.shape, rows.dtype),
        ),
        in_specs=[vmem, vmem],
        out_specs=(vmem, vmem),
        scratch_shapes=[dma((2,))] + [dma((size - 1,))] * 4,
        compiler_params=pltpu.CompilerParams(collective_id=1, has_side_effects=True),
        name="square_exchange",
    )(part, rows)


def sum_kernel(rows, landed, out, total):
    total[...] = jnp.zeros_like(total)
    for b in range(landed.shape[0]):
        for n in range(landed.shape[1]):
            total[rows[b, 0, n]] += landed[b, n].astype(jnp.float32)
    out[...] = total[...].astype(out.dtype)


def sum_products(landed, rows, count):
    shape = (count,) + landed.shape[2:]
    vmem = pl.BlockSpec(memory_space=pltpu.VMEM)
    return pl.pallas_call(
        sum_kernel,
        out_shape=jax.ShapeDtypeStruct(shape, landed.dtype),
        in_specs=[pl.BlockSpec(memory_space=pltpu.SMEM), vmem],
        out_specs=vmem,
        scratch_shapes=[pltpu.VMEM(shape, jnp.float32)],
        name="square_sum",
    )(rows, landed)


def spread_kernel(size, pieces, chunk, out, own, send, recv):
    me = lax.axis_index("gz")
    rows = chunk.shape[0] // pieces
    greet(("gz",))
    keep = pltpu.make_async_copy(chunk, out.at[me], own)
    keep.start()

    def hop(side, step, p):
        way = 1 - 2 * side
        block = me - way * step
        span = pl.ds(p * rows, rows)
        source = chunk.at[span] if step == 0 else out.at[block, span]
        copy = remote(source, out.at[block, span], send.at[side, step, p], recv.at[side, step, p],
                      "gz", lax.rem(me + way + size, size))
        ahead = me + way
        valid = (block >= 0) & (block < size) & (ahead >= 0) & (ahead < size)
        return copy, valid

    def landing(side, step, p):
        way = 1 - 2 * side
        block = me - way * (step + 1)
        span = pl.ds(p * rows, rows)
        copy = remote(out.at[block, span], out.at[block, span], send.at[side, step, p],
                      recv.at[side, step, p], "gz", lax.rem(me + way + size, size))
        return copy, (block >= 0) & (block < size)

    def send_hop(side, step, p):
        copy, valid = hop(side, step, p)

        @pl.when(valid)
        def _():
            copy.start()

    for p in range(pieces):
        for side in range(2):
            send_hop(side, 0, p)
    for step in range(size - 1):
        for p in range(pieces):
            for side in range(2):
                copy, valid = landing(side, step, p)

                @pl.when(valid)
                def _():
                    copy.wait_recv()

                if step + 1 < size - 1:
                    send_hop(side, step + 1, p)
    for step in range(size - 1):
        for p in range(pieces):
            for side in range(2):
                copy, valid = hop(side, step, p)

                @pl.when(valid)
                def _():
                    copy.wait_send()
    keep.wait()


def spread(chunk):
    size = lax.axis_size("gz")
    pieces = pieces_of(chunk.shape[0], 4)
    dma = pltpu.SemaphoreType.DMA
    vmem = pl.BlockSpec(memory_space=pltpu.VMEM)
    return pl.pallas_call(
        functools.partial(spread_kernel, size, pieces),
        out_shape=jax.ShapeDtypeStruct((size,) + chunk.shape, chunk.dtype),
        in_specs=[vmem],
        out_specs=vmem,
        scratch_shapes=[dma, dma((2, size - 1, pieces)), dma((2, size - 1, pieces))],
        compiler_params=pltpu.CompilerParams(collective_id=3, has_side_effects=True),
        name="square_spread",
    )(chunk)


def second_kernel(block, slots, groups, panel_cols, square, tiles, out, total):
    step = pl.program_id(0)
    count = total.shape[0]
    height = total.shape[1] // groups

    def rows_of(c):
        return jnp.concatenate([square[q, c] for q in range(square.shape[0])], axis=0)

    @pl.when(step == 0)
    def _():
        total[...] = jnp.zeros_like(total)

    for r in range(block):
        row = step * block + r
        base = row * slots
        rounded = rows_of(row)
        for k in range(0, slots, 2):
            held = jnp.concatenate([tiles[r, j] for j in range(k, min(k + 2, slots))], axis=1)
            product = jnp.dot(rounded, held, preferred_element_type=jnp.float32)
            for j in range(k, min(k + 2, slots)):
                width = tiles.shape[3]
                total[panel_cols[base + j]] += product[:, (j - k) * width:(j - k + 1) * width]

    @pl.when(step == pl.num_programs(0) - 1)
    def _():
        same = (lax.axis_index("gy") == lax.axis_index("gz")).astype(jnp.float32)

        @pl.loop(0, count)
        def _(c):
            value = (3.0 * same) * rows_of(c).astype(jnp.float32) - 2.0 * total[c]
            value = value.astype(out.dtype)
            for g in range(groups):
                out[g, c] = value[g * height:(g + 1) * height]


def second(square, panel, panel_cols):
    count, slots, size = panel.shape[0], panel.shape[1], panel.shape[2]
    groups = lax.axis_size("gy")
    block = pieces_of(count, 8)
    shape = (groups, count, size // groups, size)
    return pl.pallas_call(
        functools.partial(second_kernel, block, slots, groups),
        out_shape=jax.ShapeDtypeStruct(shape, panel.dtype),
        grid=(count // block,),
        in_specs=[
            pl.BlockSpec(memory_space=pltpu.SMEM),
            pl.BlockSpec(square.shape, lambda i: (0, 0, 0, 0)),
            pl.BlockSpec((block, slots, size, size), lambda i: (i, 0, 0, 0)),
        ],
        out_specs=pl.BlockSpec(shape, lambda i: (0, 0, 0, 0)),
        scratch_shapes=[pltpu.VMEM((count, size, size), jnp.float32)],
        compiler_params=pltpu.CompilerParams(dimension_semantics=("arbitrary",)),
        name="cube_partial",
    )(panel_cols, square, panel)


def scatter_kernel(size, pieces, part, out, landed, send, recv):
    me = lax.axis_index("gy")
    rows = part.shape[1] // pieces
    width = part.shape[3]
    greet(("gy",))
    copies = []
    for p in range(pieces):
        span = pl.ds(p * rows, rows)
        for d in range(1, size):
            peer = lax.rem(me + d, size)
            copy = remote(part.at[peer, span], landed.at[d - 1, p],
                          send.at[d - 1, p], recv.at[d - 1, p], "gy", peer)
            copy.start()
            copies.append(copy)
    for p in range(pieces):
        for d in range(1, size):
            copies[p * (size - 1) + d - 1].wait_recv()
        for r in range(rows):
            c = p * rows + r
            total = part[me, c].astype(jnp.float32)
            for d in range(1, size):
                total = total + landed[d - 1, p, r].astype(jnp.float32)
            out[:, c * width:(c + 1) * width] = total
    for copy in copies:
        copy.wait_send()


def scatter_result(part):
    size = lax.axis_size("gy")
    count, height, width = part.shape[1:]
    pieces = pieces_of(count, 4)
    dma = pltpu.SemaphoreType.DMA
    return pl.pallas_call(
        functools.partial(scatter_kernel, size, pieces),
        out_shape=jax.ShapeDtypeStruct((height, count * width), jnp.float32),
        in_specs=[pl.BlockSpec(memory_space=pltpu.VMEM)],
        out_specs=pl.BlockSpec(memory_space=pltpu.VMEM),
        scratch_shapes=[
            pltpu.VMEM((size - 1, pieces, count // pieces, height, width), part.dtype),
            dma((size - 1, pieces)), dma((size - 1, pieces)),
        ],
        compiler_params=pltpu.CompilerParams(collective_id=2, has_side_effects=True),
        name="result_scatter",
    )(part)


def local(block_values, block_cols):
    tiles = block_values[0, :, 0]
    cols = block_cols[0, :, 0]
    slots = cols.shape[1]
    panel, panel_cols, left, left_cols = gather(tiles, cols)
    panel_cols = panel_cols[:, :, :slots].reshape(-1)
    left_cols = left_cols[0, :slots]
    part, rows = first(left[0], left_cols, panel, panel_cols)
    landed, rows = exchange(part, rows)
    square = spread(sum_products(landed, rows, panel.shape[0]))
    return scatter_result(second(square, panel, panel_cols))


def solution(mesh):
    in_specs = (P("gy", "gx", "gz", None, None, None), P("gy", "gx", "gz", None))
    out_specs = P(("gx", "gy"), "gz")
    return jax.shard_map(local, mesh=mesh, in_specs=in_specs, out_specs=out_specs, check_vma=False)
```

```python
import functools

import jax
import jax.numpy as jnp
from jax import lax
from jax.experimental import pallas as pl
from jax.experimental.pallas import tpu as pltpu
from jax.sharding import PartitionSpec as P

WIN = 1
LANES = 128
MESH = pl.DeviceIdType.MESH


def pieces_of(count, most):
    for pieces in range(min(count, most), 0, -1):
        if count % pieces == 0:
            return pieces


def greet(axes):
    barrier = pltpu.get_barrier_semaphore()
    total = 0
    for axis in axes:
        size = lax.axis_size(axis)
        me = lax.axis_index(axis)
        for step in range(1, size):
            pl.semaphore_signal(
                barrier, inc=1, device_id={axis: lax.rem(me + step, size)}, device_id_type=MESH
            )
        total += size - 1
    pl.semaphore_wait(barrier, total)


def remote(src, dst, send, recv, axis, peer):
    return pltpu.make_async_remote_copy(
        src_ref=src, dst_ref=dst, send_sem=send, recv_sem=recv,
        device_id={axis: peer}, device_id_type=MESH,
    )


def gather_kernel(
    n_gx, n_gy, pieces, tiles, cols, panel, panel_cols, left, left_cols,
    stage, load_sem, own_sem, send_sem, recv_sem, col_own, col_send, col_recv,
    win_own, win_send, win_recv,
):
    gx, gy = lax.axis_index("gx"), lax.axis_index("gy")
    rows = tiles.shape[0]
    part = rows // pieces
    loads = []
    for p in range(pieces):
        span = pl.ds(p * part, part)
        loads.append(pltpu.make_async_copy(tiles.at[span], stage.at[span], load_sem.at[p]))
        loads[-1].start()
    greet(("gx", "gy"))
    window = stage.at[pl.ds(0, WIN)]
    col_copies = [pltpu.make_async_copy(cols, panel_cols.at[gx], col_own)]
    for step in range(1, n_gx):
        col_copies.append(
            remote(cols, panel_cols.at[gx], col_send.at[step], col_recv.at[step],
                   "gx", lax.rem(gx + step, n_gx))
        )
    for copy in col_copies:
        copy.start()
    copies = []
    for p in range(pieces):
        loads[p].wait()
        if p == 0:
            @pl.when(gy == 0)
            def _():
                for peer in range(1, n_gy):
                    remote(window, left, win_send.at[0, peer], win_recv.at[0], "gy", peer).start()
                    remote(cols, left_cols, win_send.at[1, peer], win_recv.at[1], "gy", peer).start()
                pltpu.make_async_copy(window, left, win_own.at[0]).start()
                pltpu.make_async_copy(cols, left_cols, win_own.at[1]).start()
        source = stage.at[pl.ds(p * part, part)]
        target = panel.at[pl.ds(gx * rows + p * part, part)]
        for step in range(1, n_gx):
            copy = remote(source, target, send_sem.at[step, p], recv_sem.at[step, p],
                          "gx", lax.rem(gx + step, n_gx))
            copy.start()
            copies.append(copy)
        copy = pltpu.make_async_copy(source, target, own_sem.at[p])
        copy.start()
        copies.append(copy)
    for copy in col_copies + copies:
        copy.wait()

    @pl.when(gy == 0)
    def _():
        for peer in range(1, n_gy):
            remote(window, left, win_send.at[0, peer], win_recv.at[0], "gy", peer).wait_send()
            remote(cols, left_cols, win_send.at[1, peer], win_recv.at[1], "gy", peer).wait_send()
        pltpu.make_async_copy(window, left, win_own.at[0]).wait()
        pltpu.make_async_copy(cols, left_cols, win_own.at[1]).wait()

    @pl.when(gy != 0)
    def _():
        remote(window, left, win_send.at[0, 0], win_recv.at[0], "gy", 0).wait_recv()
        remote(cols, left_cols, win_send.at[1, 0], win_recv.at[1], "gy", 0).wait_recv()


def gather(tiles, cols):
    n_gx, n_gy = lax.axis_size("gx"), lax.axis_size("gy")
    rows = tiles.shape[0]
    pieces = pieces_of(rows, 4)
    padded = jnp.pad(cols, ((0, 0), (0, LANES - cols.shape[1])))
    dma = pltpu.SemaphoreType.DMA
    return pl.pallas_call(
        functools.partial(gather_kernel, n_gx, n_gy, pieces),
        out_shape=(
            jax.ShapeDtypeStruct((n_gx * rows,) + tiles.shape[1:], tiles.dtype),
            jax.ShapeDtypeStruct((n_gx,) + padded.shape, padded.dtype),
            jax.ShapeDtypeStruct((WIN,) + tiles.shape[1:], tiles.dtype),
            jax.ShapeDtypeStruct(padded.shape, padded.dtype),
        ),
        in_specs=[
            pl.BlockSpec(memory_space=pl.ANY),
            pl.BlockSpec(memory_space=pltpu.VMEM),
        ],
        out_specs=[pl.BlockSpec(memory_space=pl.ANY)] * 4,
        scratch_shapes=[
            pltpu.VMEM(tiles.shape, tiles.dtype),
            dma((pieces,)), dma((pieces,)), dma((n_gx, pieces)), dma((n_gx, pieces)),
            dma, dma((n_gx,)), dma((n_gx,)),
            dma((2,)), dma((2, n_gy)), dma((2,)),
        ],
        compiler_params=pltpu.CompilerParams(collective_id=0, has_side_effects=True),
        name="gather_tiles",
    )(tiles, padded)


def first_kernel(
    slots, pairs, left_cols, panel_cols, left, panel, out, rows_out,
    inverse, place, which, stage, sem,
):
    groups, height = out.shape[0], out.shape[2]

    for c in range(inverse.shape[0]):
        inverse[c] = -1
    for c in range(pairs, rows_out.shape[1]):
        rows_out[0, c] = 0
    for k in range(slots):
        inverse[left_cols[0, k]] = k
    entries = panel.shape[0]
    group = pieces_of(entries, 32)

    def scan(step, found):
        base = step * group
        matches = [inverse[panel_cols[base + j]] for j in range(group)]
        for j, k in enumerate(matches):
            place[found] = base + j
            which[found] = k
            found = found + (k >= 0).astype(jnp.int32)
        return found

    lax.fori_loop(0, entries // group, scan, jnp.int32(0))
    bunch = pairs // pieces_of(pairs, 4)
    copies = []
    for n in range(pairs):
        copies.append(pltpu.make_async_copy(panel.at[place[n]], stage.at[n], sem.at[n]))
        copies[-1].start()
    for n in range(pairs):
        rows_out[0, n] = lax.div(place[n], jnp.int32(slots))
    for first_pair in range(0, pairs, bunch):
        span = range(first_pair, first_pair + bunch)
        for n in span:
            copies[n].wait()
        for n in span:
            product = lax.dot_general(
                left[which[n]], stage[n], (((1,), (1,)), ((), ())),
                preferred_element_type=jnp.float32,
            ).astype(out.dtype)
            for g in range(groups):
                out[g, n] = product[g * height:(g + 1) * height]


def first(left, left_cols, panel, panel_cols):
    count, slots, size = panel.shape[0], panel.shape[1], panel.shape[2]
    pairs = slots * slots
    groups = lax.axis_size("gz")
    smem = pl.BlockSpec(memory_space=pltpu.SMEM)
    vmem = pl.BlockSpec(memory_space=pltpu.VMEM)
    return pl.pallas_call(
        functools.partial(first_kernel, slots, pairs),
        out_shape=(
            jax.ShapeDtypeStruct((groups, pairs, size // groups, size), panel.dtype),
            jax.ShapeDtypeStruct((1, LANES), jnp.int32),
        ),
        in_specs=[smem, smem, vmem, pl.BlockSpec(memory_space=pl.ANY)],
        out_specs=(vmem, smem),
        scratch_shapes=[
            pltpu.SMEM((count,), jnp.int32),
            pltpu.SMEM((pairs + 1,), jnp.int32),
            pltpu.SMEM((pairs + 1,), jnp.int32),
            pltpu.VMEM((pairs, size, size), panel.dtype),
            pltpu.SemaphoreType.DMA((pairs,)),
        ],
        name="square_products",
    )(left_cols, panel_cols, left, panel.reshape(count * slots, size, size))


def exchange_kernel(size, part, rows, landed, rows_landed, own, send, recv, row_send, row_recv):
    me = lax.axis_index("gz")
    greet(("gz",))
    copies = [
        pltpu.make_async_copy(part.at[me], landed.at[me], own.at[0]),
        pltpu.make_async_copy(rows, rows_landed.at[me], own.at[1]),
    ]
    for d in range(1, size):
        peer = lax.rem(me + d, size)
        copies.append(remote(part.at[peer], landed.at[me], send.at[d - 1], recv.at[d - 1], "gz", peer))
        copies.append(
            remote(rows, rows_landed.at[me], row_send.at[d - 1], row_recv.at[d - 1], "gz", peer)
        )
    for copy in copies:
        copy.start()
    for copy in copies:
        copy.wait()


def exchange(part, rows):
    size = lax.axis_size("gz")
    dma = pltpu.SemaphoreType.DMA
    vmem = pl.BlockSpec(memory_space=pltpu.VMEM)
    return pl.pallas_call(
        functools.partial(exchange_kernel, size),
        out_shape=(
            jax.ShapeDtypeStruct(part.shape, part.dtype),
            jax.ShapeDtypeStruct((size,) + rows.shape, rows.dtype),
        ),
        in_specs=[vmem, vmem],
        out_specs=(vmem, vmem),
        scratch_shapes=[dma((2,))] + [dma((size - 1,))] * 4,
        compiler_params=pltpu.CompilerParams(collective_id=1, has_side_effects=True),
        name="square_exchange",
    )(part, rows)


def sum_kernel(rows, landed, out, total):
    total[...] = jnp.zeros_like(total)
    for b in range(landed.shape[0]):
        for n in range(landed.shape[1]):
            total[rows[b, 0, n]] += landed[b, n].astype(jnp.float32)
    out[...] = total[...].astype(out.dtype)


def sum_products(landed, rows, count):
    shape = (count,) + landed.shape[2:]
    vmem = pl.BlockSpec(memory_space=pltpu.VMEM)
    return pl.pallas_call(
        sum_kernel,
        out_shape=jax.ShapeDtypeStruct(shape, landed.dtype),
        in_specs=[pl.BlockSpec(memory_space=pltpu.SMEM), vmem],
        out_specs=vmem,
        scratch_shapes=[pltpu.VMEM(shape, jnp.float32)],
        name="square_sum",
    )(rows, landed)


def spread_kernel(size, pieces, chunk, out, own, send, recv):
    me = lax.axis_index("gz")
    rows = chunk.shape[0] // pieces
    greet(("gz",))
    keep = pltpu.make_async_copy(chunk, out.at[me], own)
    keep.start()

    def hop(side, step, p):
        way = 1 - 2 * side
        block = me - way * step
        span = pl.ds(p * rows, rows)
        source = chunk.at[span] if step == 0 else out.at[block, span]
        copy = remote(source, out.at[block, span], send.at[side, step, p], recv.at[side, step, p],
                      "gz", lax.rem(me + way + size, size))
        ahead = me + way
        valid = (block >= 0) & (block < size) & (ahead >= 0) & (ahead < size)
        return copy, valid

    def landing(side, step, p):
        way = 1 - 2 * side
        block = me - way * (step + 1)
        span = pl.ds(p * rows, rows)
        copy = remote(out.at[block, span], out.at[block, span], send.at[side, step, p],
                      recv.at[side, step, p], "gz", lax.rem(me + way + size, size))
        return copy, (block >= 0) & (block < size)

    def send_hop(side, step, p):
        copy, valid = hop(side, step, p)

        @pl.when(valid)
        def _():
            copy.start()

    for p in range(pieces):
        for side in range(2):
            send_hop(side, 0, p)
    for step in range(size - 1):
        for p in range(pieces):
            for side in range(2):
                copy, valid = landing(side, step, p)

                @pl.when(valid)
                def _():
                    copy.wait_recv()

                if step + 1 < size - 1:
                    send_hop(side, step + 1, p)
    for step in range(size - 1):
        for p in range(pieces):
            for side in range(2):
                copy, valid = hop(side, step, p)

                @pl.when(valid)
                def _():
                    copy.wait_send()
    keep.wait()


def spread(chunk):
    size = lax.axis_size("gz")
    pieces = pieces_of(chunk.shape[0], 8)
    dma = pltpu.SemaphoreType.DMA
    vmem = pl.BlockSpec(memory_space=pltpu.VMEM)
    return pl.pallas_call(
        functools.partial(spread_kernel, size, pieces),
        out_shape=jax.ShapeDtypeStruct((size,) + chunk.shape, chunk.dtype),
        in_specs=[vmem],
        out_specs=vmem,
        scratch_shapes=[dma, dma((2, size - 1, pieces)), dma((2, size - 1, pieces))],
        compiler_params=pltpu.CompilerParams(collective_id=3, has_side_effects=True),
        name="square_spread",
    )(chunk)


def second_kernel(block, slots, groups, panel_cols, square, tiles, out, total):
    step = pl.program_id(0)
    count = total.shape[0]
    height = total.shape[1] // groups

    def rows_of(c):
        return jnp.concatenate([square[q, c] for q in range(square.shape[0])], axis=0)

    @pl.when(step == 0)
    def _():
        total[...] = jnp.zeros_like(total)

    for r in range(block):
        row = step * block + r
        base = row * slots
        rounded = rows_of(row)
        for k in range(0, slots, 2):
            held = jnp.concatenate([tiles[r, j] for j in range(k, min(k + 2, slots))], axis=1)
            product = jnp.dot(rounded, held, preferred_element_type=jnp.float32)
            for j in range(k, min(k + 2, slots)):
                width = tiles.shape[3]
                total[panel_cols[base + j]] += product[:, (j - k) * width:(j - k + 1) * width]

    @pl.when(step == pl.num_programs(0) - 1)
    def _():
        same = (lax.axis_index("gy") == lax.axis_index("gz")).astype(jnp.float32)

        @pl.loop(0, count)
        def _(c):
            value = (3.0 * same) * rows_of(c).astype(jnp.float32) - 2.0 * total[c]
            value = value.astype(out.dtype)
            for g in range(groups):
                out[g, c] = value[g * height:(g + 1) * height]


def second(square, panel, panel_cols):
    count, slots, size = panel.shape[0], panel.shape[1], panel.shape[2]
    groups = lax.axis_size("gy")
    block = pieces_of(count, 8)
    shape = (groups, count, size // groups, size)
    return pl.pallas_call(
        functools.partial(second_kernel, block, slots, groups),
        out_shape=jax.ShapeDtypeStruct(shape, panel.dtype),
        grid=(count // block,),
        in_specs=[
            pl.BlockSpec(memory_space=pltpu.SMEM),
            pl.BlockSpec(square.shape, lambda i: (0, 0, 0, 0)),
            pl.BlockSpec((block, slots, size, size), lambda i: (i, 0, 0, 0)),
        ],
        out_specs=pl.BlockSpec(shape, lambda i: (0, 0, 0, 0)),
        scratch_shapes=[pltpu.VMEM((count, size, size), jnp.float32)],
        compiler_params=pltpu.CompilerParams(dimension_semantics=("arbitrary",)),
        name="cube_partial",
    )(panel_cols, square, panel)


def scatter_kernel(size, pieces, part, out, landed, send, recv):
    me = lax.axis_index("gy")
    rows = part.shape[1] // pieces
    width = part.shape[3]
    greet(("gy",))
    copies = []
    for p in range(pieces):
        span = pl.ds(p * rows, rows)
        for d in range(1, size):
            peer = lax.rem(me + d, size)
            copy = remote(part.at[peer, span], landed.at[d - 1, p],
                          send.at[d - 1, p], recv.at[d - 1, p], "gy", peer)
            copy.start()
            copies.append(copy)
    for p in range(pieces):
        for d in range(1, size):
            copies[p * (size - 1) + d - 1].wait_recv()
        for r in range(rows):
            c = p * rows + r
            total = part[me, c].astype(jnp.float32)
            for d in range(1, size):
                total = total + landed[d - 1, p, r].astype(jnp.float32)
            out[:, c * width:(c + 1) * width] = total
    for copy in copies:
        copy.wait_send()


def scatter_result(part):
    size = lax.axis_size("gy")
    count, height, width = part.shape[1:]
    pieces = pieces_of(count, 8)
    dma = pltpu.SemaphoreType.DMA
    return pl.pallas_call(
        functools.partial(scatter_kernel, size, pieces),
        out_shape=jax.ShapeDtypeStruct((height, count * width), jnp.float32),
        in_specs=[pl.BlockSpec(memory_space=pltpu.VMEM)],
        out_specs=pl.BlockSpec(memory_space=pltpu.VMEM),
        scratch_shapes=[
            pltpu.VMEM((size - 1, pieces, count // pieces, height, width), part.dtype),
            dma((size - 1, pieces)), dma((size - 1, pieces)),
        ],
        compiler_params=pltpu.CompilerParams(collective_id=2, has_side_effects=True),
        name="result_scatter",
    )(part)


def local(block_values, block_cols):
    tiles = block_values[0, :, 0]
    cols = block_cols[0, :, 0]
    slots = cols.shape[1]
    panel, panel_cols, left, left_cols = gather(tiles, cols)
    panel_cols = panel_cols[:, :, :slots].reshape(-1)
    part, rows = first(left[0], left_cols, panel, panel_cols)
    landed, rows = exchange(part, rows)
    square = spread(sum_products(landed, rows, panel.shape[0]))
    return scatter_result(second(square, panel, panel_cols))


def solution(mesh):
    in_specs = (P("gy", "gx", "gz", None, None, None), P("gy", "gx", "gz", None))
    out_specs = P(("gx", "gy"), "gz")
    return jax.shard_map(local, mesh=mesh, in_specs=in_specs, out_specs=out_specs, check_vma=False)
```
